32 devices in a mesh: dom: 16 (over z, y, core), ch: 2 (over x).
Axes of the slice: x: 2, y: 2, z: 4, core: 2. Of those that a mesh axis runs over, the one named last changes fastest.
Arguments:
- node_irreps: bfloat16 [49, 128, 256], P(None, 'ch', 'dom'), may hold values from -6 to 6
- out_grad: bfloat16 [49, 128, 256], P(None, 'ch', 'dom'), may hold values from -6 to 6
- edge_source: int32 [8, 256], P(None, 'dom'), may hold values from 0 to 31
- edge_rotation: int32 [8, 256], P(None, 'dom'), may hold values from 0 to 255
- edge_count: int32 [256], P('dom'), may hold values from 1 to 8
- ghost_slot: int32 [256], P('dom'), may hold values from 0 to 15, as said below
- wigner: float32 [455, 4096], P(None, 'dom'), may hold values from -1 to 1, as said below
- so2_m0: bfloat16 [7, 128, 7, 128], P(None, 'ch'), may hold values from -0.1875 to 0.1875
- so2_m1: bfloat16 [2, 6, 128, 6, 128], P(None, None, 'ch'), may hold values from -0.15625 to 0.15625
- so2_m2: bfloat16 [2, 5, 128, 5, 128], P(None, None, 'ch'), may hold values from -0.15625 to 0.15625
- attn_vector: float32 [128], P('ch'), may hold values from -60 to 60
Outputs:
- updated: bfloat16 [49, 128, 256], P(None, 'ch', 'dom')
- irreps_grad: float32 [49, 128, 256], P(None, 'ch', 'dom')
The draws below stay inside these ranges and needn't reach their ends.
Inputs may be any that keep to these rules, and one draw needn't show every extreme that they name: `edge_source`: slots below 16 are the domain's own atoms in order; slot 16 + g is the domain's ghost g. `edge_rotation`: picks one of the 256 columns of wigner that belong to the atom's domain. Slots j < edge_count[a] are live, the others padding. `ghost_slot`: of a domain's 16 entries, the first 8 name atoms of the previous domain (cyclically) among its last 16 slots, the others atoms of the next domain among its first 16 slots. `wigner`: each column holds for l = 0..6 an orthogonal (2l+1) x (2l+1) block, row-major, blocks in order of l.
All inputs are finite; a program needn't handle non-finite values.
Results may differ from the reference program's by a relative error of at most 0.012.
The reference program's roundings to bfloat16 on the way (of `rot`) count: a program that leaves them out, or rounds other values in their place, can miss the bound.
Values may be sent and summed in bfloat16 or wider, within the bound.
No kernel may reach another device: no remote copies, remote signals or barrier semaphores. Data moves between devices by JAX's collectives and lax.ppermute only.
A program may use at most 128 MiB of HBM per device.

```python
import jax
import jax.numpy as jnp
from jax import lax

C = 128
HEADS = 8
LMAX = 6
MMAX = 2
OWN = 16
NB = 8
GH = 16
RIM = 16
ROT_DOM = 256
K = 49
HEAD_CH = 16
ATOMS = 256
ROTATIONS = 4096
N_DOM = 16
N_CH = 2


def draw_ghost_slot(key, part):
    half = GH // 2
    low = jax.random.randint(jax.random.fold_in(key, 101), (N_DOM, half), OWN - RIM, OWN, dtype=jnp.int32)
    high = jax.random.randint(jax.random.fold_in(key, 102), (N_DOM, GH - half), 0, RIM, dtype=jnp.int32)
    return jnp.concatenate([low, high], 1).reshape(N_DOM * GH)


def draw_wigner(key, part):
    pieces = []
    for level in range(LMAX + 1):
        width = 2 * level + 1
        raw = jax.random.normal(jax.random.fold_in(key, 211 + level), (ROTATIONS, width, width), jnp.float32) * 0.6
        skewed = raw - jnp.swapaxes(raw, 1, 2)
        eye = jnp.broadcast_to(jnp.eye(width, dtype=jnp.float32), (ROTATIONS, width, width))
        ortho = jnp.linalg.solve(eye + skewed, eye - skewed)
        pieces.append(ortho.reshape(ROTATIONS, width * width).T)
    return jnp.concatenate(pieces, 0).astype(jnp.float32)


def draw_attn_vector(key, part):
    base = jnp.clip(jax.random.normal(jax.random.fold_in(key, 301), (C,), jnp.float32), -4.0, 4.0) * HEAD_CH ** (-0.5)
    return base.astype(jnp.float32)


def touch_ends(result, key, low, high):
    spot = [jax.random.randint(jax.random.fold_in(key, axis), (), 0, length) for axis, length in enumerate(result.shape)]
    longest = result.shape.index(max(result.shape))
    beside = spot[:longest] + [(spot[longest] + 1) % result.shape[longest]] + spot[longest + 1:]
    return result.at[tuple(spot)].set(low).at[tuple(beside)].set(high)


def level_of(key, dims, cuts, least, top_value):
    gain = 1.0
    for dim, blocks in cuts:
        heights = jax.random.uniform(jax.random.fold_in(jax.random.fold_in(key, 6), dim), (blocks,), jnp.float32, least / len(cuts), top_value / len(cuts))
        gain = gain * jnp.repeat(jnp.exp(heights), dims[dim] // blocks).reshape((-1,) + (1,) * (len(dims) - 1 - dim))
    return gain


def noise(key, shape, scale, most, split=(), kind=jnp.bfloat16):
    drawn = jax.random.normal(key, shape, jnp.float32) * scale
    if len(split) > 0:
        drawn = level_of(key, shape, split, -0.22, 0.18) * drawn
    return jnp.clip(drawn, min=-most, max=most).astype(kind)


def setup_inputs(seed: int = 0) -> dict:
    key_of = jax.random.split(jax.random.key(seed), 12)
    return {
        "node_irreps": noise(key_of[0], (K, C, ATOMS), 1.0, 6.0, ((1, 2), (2, 16))),
        "out_grad": noise(key_of[1], (K, C, ATOMS), 1.0, 6.0, ((1, 2), (2, 16))),
        "edge_source": touch_ends(jax.random.randint(key_of[2], (NB, ATOMS), 0, OWN + GH), jax.random.fold_in(key_of[2], 1), 0, (OWN + GH) - 1).astype(jnp.int32),
        "edge_rotation": touch_ends(jax.random.randint(key_of[3], (NB, ATOMS), 0, ROT_DOM), jax.random.fold_in(key_of[3], 1), 0, ROT_DOM - 1).astype(jnp.int32),
        "edge_count": touch_ends(jax.random.randint(key_of[4], (ATOMS,), 1, NB + 1), jax.random.fold_in(key_of[4], 1), 1, NB).astype(jnp.int32),
        "ghost_slot": draw_ghost_slot(jax.random.fold_in(key_of[11], 71), 0),
        "wigner": draw_wigner(jax.random.fold_in(key_of[11], 71), 0),
        "so2_m0": noise(key_of[7], (LMAX + 1, C, LMAX + 1, C), ((LMAX + 1) * C) ** -0.5, 0.1875, ((1, 2),)),
        "so2_m1": noise(key_of[8], (2, LMAX, C, LMAX, C), (2 * LMAX * C) ** -0.5, 0.15625, ((2, 2),)),
        "so2_m2": noise(key_of[9], (2, LMAX - 1, C, LMAX - 1, C), (2 * (LMAX - 1) * C) ** -0.5, 0.15625, ((2, 2),)),
        "attn_vector": draw_attn_vector(jax.random.fold_in(key_of[11], 71), 0),
    }


def plan_tables(degree_top, order_top):
    blocks = []
    offset = 0
    lmajor = []
    for level in range(degree_top + 1):
        width = 2 * level + 1
        reach = min(level, order_top)
        kept = [level + order for order in range(-reach, reach + 1)]
        blocks.append((level, width, offset, kept))
        for order in range(-reach, reach + 1):
            lmajor.append((level, order))
        offset += width * width
    grouped = [(level, 0) for level in range(degree_top + 1)]
    for order in range(1, order_top + 1):
        grouped += [(level, order) for level in range(order, degree_top + 1)]
        grouped += [(level, -order) for level in range(order, degree_top + 1)]
    to_group = [lmajor.index(entry) for entry in grouped]
    to_major = [grouped.index(entry) for entry in lmajor]
    return (blocks, to_group, to_major)

def rotate_in(feats, wig_edges, blocks, to_group):
    parts = []
    for level, width, offset, kept in blocks:
        for row in kept:
            acc = wig_edges[offset + row * width][None, :] * feats[level * level]
            for col in range(1, width):
                acc = acc + wig_edges[offset + row * width + col][None, :] * feats[level * level + col]
            parts.append(acc)
    return jnp.stack([parts[i] for i in to_group])

def rotate_out(values, wig_edges, blocks, to_major):
    rows = [values[i] for i in to_major]
    out = []
    pos = 0
    for level, width, offset, kept in blocks:
        mine = rows[pos:pos + len(kept)]
        pos += len(kept)
        for col in range(width):
            acc = wig_edges[offset + kept[0] * width + col][None, :] * mine[0]
            for j in range(1, len(kept)):
                acc = acc + wig_edges[offset + kept[j] * width + col][None, :] * mine[j]
            out.append(acc)
    return jnp.stack(out)

def so2_mix(rot, w_zero, w_one, w_two, degree_top):
    chans = rot.shape[1]
    edges = rot.shape[2]
    group = w_zero.shape[1]
    first = degree_top + 1
    outs = [jnp.dot(w_zero.reshape(first * group, first * chans).astype(jnp.float32), rot[:first].reshape(first * chans, edges).astype(jnp.float32), preferred_element_type=jnp.float32).reshape(first, group, edges)]
    pos = first
    for order, weights in ((1, w_one), (2, w_two)):
        count = degree_top + 1 - order
        plus = rot[pos:pos + count].reshape(count * chans, edges)
        minus = rot[pos + count:pos + 2 * count].reshape(count * chans, edges)
        real = weights[0].reshape(count * group, count * chans)
        imag = weights[1].reshape(count * group, count * chans)
        y_plus = jnp.dot(real.astype(jnp.float32), plus.astype(jnp.float32), preferred_element_type=jnp.float32) - jnp.dot(imag.astype(jnp.float32), minus.astype(jnp.float32), preferred_element_type=jnp.float32)
        y_minus = jnp.dot(real.astype(jnp.float32), minus.astype(jnp.float32), preferred_element_type=jnp.float32) + jnp.dot(imag.astype(jnp.float32), plus.astype(jnp.float32), preferred_element_type=jnp.float32)
        outs += [y_plus.reshape(count, group, edges), y_minus.reshape(count, group, edges)]
        pos += 2 * count
    return jnp.concatenate(outs, 0)

def attend_tail(rot32, wig_edges, counts, w_zero, w_one, w_two, attn, heads_here, blocks, to_major, degree_top):
    rot = rot32.astype(jnp.bfloat16)
    mixed = so2_mix(rot, w_zero, w_one, w_two, degree_top)
    scalar = mixed[0]
    values = mixed * jax.nn.sigmoid(scalar)[None]
    group, edges = scalar.shape
    atoms_here = counts.shape[0]
    slots = edges // atoms_here
    score = (jax.nn.silu(scalar) * attn[:, None]).reshape(heads_here, group // heads_here, edges).sum(1)
    score = score.reshape(heads_here, slots, atoms_here)
    live = (lax.broadcasted_iota(jnp.int32, (slots, atoms_here), 0) < counts[None, :])[None]
    top = lax.optimization_barrier(jnp.max(jnp.where(live, score, -1e+30), axis=1, keepdims=True))
    weight = jnp.exp(jnp.where(live, score - top, -1e+30))
    weight = weight / lax.optimization_barrier(jnp.sum(weight, axis=1, keepdims=True))
    spread = jnp.broadcast_to(weight.reshape(heads_here, 1, edges), (heads_here, group // heads_here, edges)).reshape(group, edges)
    back = rotate_out(values * spread[None], wig_edges, blocks, to_major)
    return back.reshape(back.shape[0], group, slots, atoms_here).sum(2)

def reference(node_irreps, out_grad, edge_source, edge_rotation, edge_count, ghost_slot, wigner, so2_m0, so2_m1, so2_m2, attn_vector):
    blocks, to_group, to_major = plan_tables(LMAX, MMAX)
    group = C // N_CH
    heads_here = HEADS // N_CH
    slots = ghost_slot.reshape(N_DOM, GH)
    half = GH // 2

    def one_domain(x32, d):
        lower = jnp.mod(d - 1, N_DOM).astype(jnp.int32)
        upper = jnp.mod(d + 1, N_DOM).astype(jnp.int32)
        own = lax.dynamic_slice_in_dim(x32, (d * OWN).astype(jnp.int32), OWN, 2)
        below = jnp.take(lax.dynamic_slice_in_dim(x32, (lower * OWN).astype(jnp.int32), OWN, 2), slots[d, :half], axis=2)
        above = jnp.take(lax.dynamic_slice_in_dim(x32, (upper * OWN).astype(jnp.int32), OWN, 2), slots[d, half:], axis=2)
        table = jnp.concatenate([own, below, above], 2)
        source = lax.dynamic_slice_in_dim(edge_source, (d * OWN).astype(jnp.int32), OWN, 1).reshape(-1)
        turn = lax.dynamic_slice_in_dim(edge_rotation, (d * OWN).astype(jnp.int32), OWN, 1).reshape(-1)
        counts = lax.dynamic_slice_in_dim(edge_count, (d * OWN).astype(jnp.int32), OWN, 0)
        table_rot = lax.dynamic_slice_in_dim(wigner, (d * ROT_DOM).astype(jnp.int32), ROT_DOM, 1)
        wig_edges = jnp.take(table_rot, turn, axis=1)
        feats = jnp.take(table, source, axis=2)
        outs = []
        for index in range(N_CH):
            lo = index * group
            rot32 = rotate_in(feats, wig_edges, blocks, to_group)
            outs.append(attend_tail(rot32, wig_edges, counts, so2_m0[:, lo:lo + group], so2_m1[:, :, lo:lo + group], so2_m2[:, :, lo:lo + group], attn_vector[lo:lo + group], heads_here, blocks, to_major, LMAX))
        return jnp.concatenate(outs, 1)

    def forward(x32):
        stacked = lax.map(lambda d: jax.checkpoint(one_domain)(x32, d), jnp.arange(N_DOM, dtype=jnp.int32))
        return jnp.transpose(stacked, (1, 2, 0, 3)).reshape(K, C, ATOMS)
    x32 = node_irreps.astype(jnp.float32)
    agg, pullback = jax.vjp(forward, x32)
    updated = (x32 + agg).astype(jnp.bfloat16)
    grad32 = out_grad.astype(jnp.float32)
    irreps_grad = grad32 + pullback(grad32)[0]
    return (updated, irreps_grad)
```

```python
import functools

import jax
import jax.numpy as jnp
from jax import lax
from jax.experimental import pallas as pl
from jax.experimental.pallas import tpu as pltpu
from jax.sharding import PartitionSpec as P

HEADS = 8
LMAX = 6
MMAX = 2
F32 = jnp.float32
BF16 = jnp.bfloat16
HIGH = lax.Precision.HIGHEST
NT = (((1,), (1,)), ((), ()))
NN = (((1,), (0,)), ((), ()))


def dot(a, b, dims=NN, precision=None):
    return lax.dot_general(a, b, dims, precision=precision, preferred_element_type=F32)


def kept_rows():
    rows = {}
    place = 0
    offset = 0
    for level in range(LMAX + 1):
        width = 2 * level + 1
        reach = min(level, MMAX)
        for order in range(-reach, reach + 1):
            rows[level, order] = (place, offset + (level + order) * width, width)
            place += width
        offset += width * width
    return rows, place


ROWS, N_ROWS = kept_rows()
GROUPS = ((0, 0), (1, 1), (1, -1), (2, 2), (2, -2))


def plane_index():
    index = {}
    for least, order in GROUPS:
        for level in range(least, LMAX + 1):
            index[level, order] = len(index)
    return index


PLANES = plane_index()
K = (LMAX + 1) ** 2


def vmem(n):
    return [pl.BlockSpec(memory_space=pltpu.VMEM)] * n


def params(mib):
    return pltpu.CompilerParams(vmem_limit_bytes=mib * 1024 * 1024)


def column(table, slots, atoms):
    edges = slots * atoms
    row = lax.broadcasted_iota(jnp.int32, (edges, slots), 0)
    col = lax.broadcasted_iota(jnp.int32, (edges, slots), 1)
    pick = ((row >= col * atoms) & (row < (col + 1) * atoms)).astype(F32)
    spread = dot(pick, table.astype(F32), precision=HIGH)
    row = lax.broadcasted_iota(jnp.int32, (edges, atoms), 0)
    col = lax.broadcasted_iota(jnp.int32, (edges, atoms), 1)
    return jnp.sum(jnp.where(lax.rem(row, atoms) == col, spread, 0.0), axis=1, keepdims=True)


def onehot(values, width):
    edges = values.shape[0]
    lanes = lax.broadcasted_iota(jnp.int32, (edges, width), 1).astype(F32)
    return jnp.where(lanes == values, 1.0, 0.0).astype(F32)


def merge_kernel(shards, *refs):
    mine, others, full = refs[0], refs[1:-1], refs[-1]
    group = mine.shape[2]
    me = lax.axis_index("ch")
    pieces = [mine[...]] + [ref[...] for ref in others]
    for chunk in range(shards):
        value = pieces[0]
        for step in range(1, shards):
            value = jnp.where(lax.rem(me + step, shards) == chunk, pieces[step], value)
        full[:, :, chunk * group : (chunk + 1) * group] = value


def table_kernel(wigner, rotation, out_grad, dtab, g0, g1, g2, g3, g4, turned):
    slots, atoms = rotation.shape
    pick = onehot(column(rotation[...], slots, atoms), wigner.shape[1]).astype(BF16)
    wig = wigner[...]
    high = wig.astype(BF16)
    rest = wig - high.astype(F32)
    mid = rest.astype(BF16)
    low = (rest - mid.astype(F32)).astype(BF16)
    turned[...] = dot(pick, high, NT) + dot(pick, mid, NT) + dot(pick, low, NT)
    group = out_grad.shape[2]
    lanes = dtab.shape[2]
    outs = (g0, g1, g2, g3, g4)

    def step(slot, carry):
        here = pl.ds(pl.multiple_of(slot * atoms, atoms), atoms)
        mine = turned[here, :]
        for which, (least, order) in enumerate(GROUPS):
            parts = []
            for level in range(least, LMAX + 1):
                place, first, width = ROWS[level, order]
                acc = None
                for col in range(width):
                    entry = jnp.broadcast_to(mine[:, first + col : first + col + 1], (atoms, lanes))
                    dtab[place + col, here, :] = entry
                    term = entry[:, :group] * out_grad[level * level + col].astype(F32)
                    acc = term if acc is None else acc + term
                parts.append(acc)
            outs[which][here, :] = jnp.concatenate(parts, axis=1)
        return carry

    lax.fori_loop(0, slots, step, 0)


def rotate_in(slot, atoms, feats, dtab, rot):
    here = pl.ds(pl.multiple_of(slot * atoms, atoms), atoms)
    for level in range(LMAX + 1):
        width = 2 * level + 1
        planes = [feats[level * level + col, here, :] for col in range(width)]
        reach = min(level, MMAX)
        for order in range(-reach, reach + 1):
            place = ROWS[level, order][0]
            acc = dtab[place, here, :] * planes[0]
            for col in range(1, width):
                acc = acc + dtab[place + col, here, :] * planes[col]
            rot[PLANES[level, order], here, :] = acc.astype(BF16)


def rotate_out(slot, atoms, load, dtab, store):
    here = pl.ds(pl.multiple_of(slot * atoms, atoms), atoms)
    for level in range(LMAX + 1):
        width = 2 * level + 1
        reach = min(level, MMAX)
        orders = range(-reach, reach + 1)
        planes = {order: load(level, order, here) for order in orders}
        for col in range(width):
            acc = None
            for order in orders:
                term = dtab[ROWS[level, order][0] + col, here, :] * planes[order]
                acc = term if acc is None else acc + term
            store(level * level + col, here, acc)


def side(array, axis):
    return jnp.concatenate(array, axis=axis)


def edge_kernel(
    full, lower, upper, source, ghost, counts, dtab, g0, g1, g2, g3, g4, w0, w1, w2, attn,
    heads_here,
    own_out, prev_out, next_out, v0, v1, v2, v3, v4,
    feats, rot, drot, dfeats,
):
    slots, atoms = source.shape
    edges = slots * atoms
    chans = full.shape[2]
    group = w0.shape[2]
    half = ghost.shape[1] // 2
    slot_pick = onehot(column(source[...], slots, atoms), atoms + 2 * half).astype(BF16)
    row = lax.broadcasted_iota(jnp.int32, (2 * half, 2 * half), 0)
    col = lax.broadcasted_iota(jnp.int32, (2 * half, 2 * half), 1)
    ghosts = jnp.sum(jnp.where(row == col, ghost[...].astype(F32), 0.0), axis=1, keepdims=True)
    rows = lax.broadcasted_iota(jnp.int32, (2 * half, 1), 0)
    ghosts = ghosts + jnp.where(rows < half, atoms, 2 * atoms).astype(F32)
    own_row = lax.broadcasted_iota(jnp.int32, (atoms, 1), 0).astype(F32)
    places = onehot(side([own_row, ghosts], 0), 3 * atoms).astype(BF16)
    pick32 = dot(slot_pick, places)
    pick = pick32.astype(BF16)
    pick_back = jnp.transpose(pick32).astype(BF16)

    for first in range(0, K, 2):
        ks = [k for k in (first, first + 1) if k < K]
        table = side([side([full[k], lower[k], upper[k]], 0) for k in ks], 1)
        got = dot(pick, table)
        for at, k in enumerate(ks):
            feats[k] = got[:, at * chans : (at + 1) * chans]

    def in_step(slot, carry):
        rotate_in(slot, atoms, feats, dtab, rot)
        return carry

    lax.fori_loop(0, slots, in_step, 0)

    def planes_of(which):
        least, order = GROUPS[which]
        return side([rot[PLANES[level, order]] for level in range(least, LMAX + 1)], 1)

    def weights_of(ref):
        count = ref.shape[-3]
        lead = ref.shape[-2] * count * (ref.shape[0] if len(ref.shape) == 5 else 1)
        if len(ref.shape) == 4:
            parts = [ref[:, level].reshape(lead, chans) for level in range(count)]
        else:
            parts = [ref[:, :, level].reshape(lead, chans) for level in range(count)]
        return side(parts, 1)

    y0 = dot(planes_of(0), weights_of(w0), NT)

    def mixed(which, ref):
        both = dot(side([planes_of(which), planes_of(which + 1)], 0), weights_of(ref), NT)
        wide = both.shape[1] // 2
        plus = both[:edges, :wide] - both[edges:, wide:]
        minus = both[edges:, :wide] + both[:edges, wide:]
        return plus, minus

    y1, y2 = mixed(1, w1)
    y3, y4 = mixed(3, w2)
    mixes = (y0, y1, y2, y3, y4)
    grads = (g0[...], g1[...], g2[...], g3[...], g4[...])

    scalar = y0[:, :group]
    sig = 1.0 / (1.0 + jnp.exp(-scalar))
    width = group // heads_here
    head_row = lax.broadcasted_iota(jnp.int32, (group, group), 0) // width
    head_col = lax.broadcasted_iota(jnp.int32, (group, group), 1) // width
    same_head = jnp.where(head_row == head_col, 1.0, 0.0).astype(F32)
    vector = attn[...]
    silu = scalar * sig
    score = dot(silu * vector, same_head, precision=HIGH).reshape(slots, atoms, group)
    cnt = jnp.broadcast_to(counts[...], (slots, atoms))
    slot_no = lax.broadcasted_iota(jnp.int32, (slots, atoms), 0)
    live = (column(slot_no < cnt, slots, atoms) > 0.5)
    live = jnp.broadcast_to(live, (edges, group)).reshape(slots, atoms, group)
    score = jnp.where(live, score, -1e30)
    top = jnp.max(score, axis=0, keepdims=True)
    weight = jnp.where(live, jnp.exp(score - top), 0.0)
    weight = weight / jnp.sum(weight, axis=0, keepdims=True)
    flat = weight.reshape(edges, group)
    factor = flat * sig

    overlap = None
    for grad, mix in zip(grads, mixes):
        both = grad * mix
        for at in range(0, both.shape[1], group):
            piece = both[:, at : at + group]
            overlap = piece if overlap is None else overlap + piece
    dweight = dot(overlap * sig, same_head, precision=HIGH).reshape(slots, atoms, group)
    mean = jnp.sum(weight * dweight, axis=0, keepdims=True)
    dscore = (weight * (dweight - mean)).reshape(edges, group)
    dscalar = overlap * factor * (1.0 - sig) + dscore * vector * sig * (1.0 + scalar * (1.0 - sig))

    dmix = []
    for grad, mix, out in zip(grads, mixes, (v0, v1, v2, v3, v4)):
        wide = side([factor] * (mix.shape[1] // group), 1)
        out[...] = mix * wide
        dmix.append(grad * wide)
    head = dmix[0][:, :group] + dscalar
    back0 = side([head, dmix[0][:, group:]], 1).astype(BF16)

    def keep(which, value, first=0):
        least, order = GROUPS[which]
        for at, level in enumerate(range(least, LMAX + 1)):
            drot[PLANES[level, order]] = (
                value[:, at * chans : (at + 1) * chans].astype(BF16).astype(F32)
            )

    keep(0, dot(back0, weights_of(w0)))
    for which, ref in ((1, w1), (3, w2)):
        plus, minus = dmix[which], dmix[which + 1]
        stacked = side([side([plus, minus], 1), side([minus, -plus], 1)], 0).astype(BF16)
        both = dot(stacked, weights_of(ref))
        keep(which, both[:edges])
        keep(which + 1, both[edges:])

    def load(level, order, here):
        return drot[PLANES[level, order], here, :]

    def store(k, here, value):
        dfeats[k, here, :] = value.astype(BF16)

    def out_step(slot, carry):
        rotate_out(slot, atoms, load, dtab, store)
        return carry

    lax.fori_loop(0, slots, out_step, 0)

    for first in range(0, K, 2):
        ks = [k for k in (first, first + 1) if k < K]
        got = dot(pick_back, side([dfeats[k] for k in ks], 1))
        for at, k in enumerate(ks):
            mine = got[:, at * chans : (at + 1) * chans]
            own_out[k] = mine[:atoms]
            prev_out[k] = mine[atoms : 2 * atoms].astype(BF16)
            next_out[k] = mine[2 * atoms :].astype(BF16)


def update_kernel(v0, v1, v2, v3, v4, dtab, mine, out, agg):
    atoms, group = mine.shape[1], mine.shape[2]
    slots = dtab.shape[1] // atoms
    values = (v0, v1, v2, v3, v4)
    lanes = dtab.shape[2]
    agg[...] = jnp.zeros_like(agg)

    def step(slot, carry):
        here = pl.ds(pl.multiple_of(slot * atoms, atoms), atoms)
        wide = [ref[here, :] for ref in values]
        for level in range(LMAX + 1):
            reach = min(level, MMAX)
            planes = {}
            for which, (least, order) in enumerate(GROUPS):
                if least <= level:
                    at = (level - least) * group
                    planes[order] = wide[which][:, at : at + group]
            for col in range(2 * level + 1):
                acc = agg[level * level + col]
                for order in range(-reach, reach + 1):
                    entry = dtab[ROWS[level, order][0] + col, here, :]
                    acc = acc + entry[:, :group] * planes[order]
                agg[level * level + col] = acc
        return carry

    lax.fori_loop(0, slots, step, 0)
    out[...] = (mine[...].astype(F32) + agg[...]).astype(BF16)


def settle_kernel(shards, own, above, below, out_grad, mine_out, *others):
    group = out_grad.shape[2]
    me = lax.axis_index("ch")
    total = own[...] + above[...].astype(F32) + below[...].astype(F32)
    for step in range(shards):
        wanted = lax.rem(me + step, shards)
        value = total[:, :, :group]
        for chunk in range(1, shards):
            value = jnp.where(wanted == chunk, total[:, :, chunk * group : (chunk + 1) * group], value)
        if step == 0:
            mine_out[...] = value + out_grad[...].astype(F32)
        else:
            others[step - 1][...] = value.astype(BF16)


def shift(array, axis, by):
    count = lax.axis_size(axis)
    return lax.ppermute(array, axis, [(i, (i + by) % count) for i in range(count)])


def cost(flops, size):
    return pl.CostEstimate(flops=flops, bytes_accessed=size, transcendentals=0)


def on_device(
    node_irreps, out_grad, edge_source, edge_rotation, edge_count, ghost_slot, wigner,
    so2_m0, so2_m1, so2_m2, attn_vector,
):
    group, atoms = node_irreps.shape[1], node_irreps.shape[2]
    shards = lax.axis_size("ch")
    chans = group * shards
    slots = edge_source.shape[0]
    edges = slots * atoms
    heads_here = HEADS // shards
    shape = jax.ShapeDtypeStruct
    mine = jnp.transpose(node_irreps, (0, 2, 1))
    grad = jnp.transpose(out_grad, (0, 2, 1))
    w0 = jnp.transpose(so2_m0, (0, 2, 1, 3))
    w1 = jnp.transpose(so2_m1, (0, 1, 3, 2, 4))
    w2 = jnp.transpose(so2_m2, (0, 1, 3, 2, 4))

    others = [shift(mine, "ch", -step) for step in range(1, shards)]
    full = pl.pallas_call(
        functools.partial(merge_kernel, shards),
        out_shape=shape((K, atoms, chans), BF16),
        in_specs=vmem(shards),
        out_specs=vmem(1)[0],
        compiler_params=params(4),
        name="merge",
    )(mine, *others)
    lower = shift(full, "dom", 1)
    upper = shift(full, "dom", -1)

    widths = [(LMAX + 1 - least) * group for least, _ in GROUPS]
    dtab, *grads = pl.pallas_call(
        table_kernel,
        out_shape=[shape((N_ROWS, edges, chans), F32)] + [shape((edges, w), F32) for w in widths],
        in_specs=vmem(3),
        out_specs=vmem(6),
        scratch_shapes=[pltpu.VMEM((edges, wigner.shape[0]), F32)],
        compiler_params=params(24),
        cost_estimate=cost(50_000_000, 16_000_000),
        name="tables",
    )(wigner, edge_rotation, grad)

    body = lambda *refs: edge_kernel(*refs[:16], heads_here, *refs[16:])
    own, to_prev, to_next, *values = pl.pallas_call(
        body,
        out_shape=[
            shape((K, atoms, chans), F32),
            shape((K, atoms, chans), BF16),
            shape((K, atoms, chans), BF16),
        ] + [shape((edges, w), F32) for w in widths],
        in_specs=vmem(16),
        out_specs=vmem(8),
        scratch_shapes=[
            pltpu.VMEM((K, edges, chans), F32),
            pltpu.VMEM((len(PLANES), edges, chans), BF16),
            pltpu.VMEM((len(PLANES), edges, chans), F32),
            pltpu.VMEM((K, edges, chans), BF16),
        ],
        compiler_params=params(40),
        cost_estimate=cost(2_000_000_000, 20_000_000),
        name="edges",
    )(
        full, lower, upper, edge_source, ghost_slot.reshape(1, -1), edge_count.reshape(1, -1),
        dtab, *grads, w0, w1, w2, attn_vector.reshape(1, -1),
    )
    above = shift(to_prev, "dom", -1)
    below = shift(to_next, "dom", 1)

    updated = pl.pallas_call(
        update_kernel,
        out_shape=shape((K, atoms, group), BF16),
        in_specs=vmem(7),
        out_specs=vmem(1)[0],
        scratch_shapes=[pltpu.VMEM((K, atoms, group), F32)],
        compiler_params=params(24),
        cost_estimate=cost(20_000_000, 16_000_000),
        name="update",
    )(*values, dtab, mine)

    mine_grad, *sent = pl.pallas_call(
        functools.partial(settle_kernel, shards),
        out_shape=[shape((K, atoms, group), F32)] + [shape((K, atoms, group), BF16)] * (shards - 1),
        in_specs=vmem(4),
        out_specs=vmem(shards),
        compiler_params=params(8),
        name="settle",
    )(own, above, below, grad)
    for step in range(1, shards):
        mine_grad = mine_grad + shift(sent[step - 1], "ch", step).astype(F32)
    return (jnp.transpose(updated, (0, 2, 1)), jnp.transpose(mine_grad, (0, 2, 1)))


def solution(mesh):
    placed = (
        P(None, "ch", "dom"), P(None, "ch", "dom"), P(None, "dom"), P(None, "dom"), P("dom"),
        P("dom"), P(None, "dom"), P(None, "ch", None, None), P(None, None, "ch", None, None),
        P(None, None, "ch", None, None), P("ch"),
    )
    return jax.shard_map(
        on_device,
        mesh=mesh,
        in_specs=placed,
        out_specs=(P(None, "ch", "dom"), P(None, "ch", "dom")),
        check_vma=False,
    )
```

```python
import functools

import jax
import jax.numpy as jnp
from jax import lax
from jax.experimental import pallas as pl
from jax.experimental.pallas import tpu as pltpu
from jax.sharding import PartitionSpec as P

HEADS = 8
LMAX = 6
MMAX = 2
F32 = jnp.float32
BF16 = jnp.bfloat16
HIGH = lax.Precision.HIGHEST
NT = (((1,), (1,)), ((), ()))
NN = (((1,), (0,)), ((), ()))
TN = (((0,), (0,)), ((), ()))
BLOCK = 16


def dot(a, b, dims=NN, precision=None):
    return lax.dot_general(a, b, dims, precision=precision, preferred_element_type=F32)


def kept_rows():
    rows = {}
    offset = 0
    for level in range(LMAX + 1):
        width = 2 * level + 1
        reach = min(level, MMAX)
        for order in range(-reach, reach + 1):
            rows[level, order] = offset + (level + order) * width
        offset += width * width
    return rows


ROWS = kept_rows()
K = (LMAX + 1) ** 2


def vmem(n):
    return [pl.BlockSpec(memory_space=pltpu.VMEM)] * n


def hbm():
    return pl.BlockSpec(memory_space=pltpu.MemorySpace.HBM)


def pinned(array):
    return pltpu.with_memory_space_constraint(array, pltpu.MemorySpace.HBM)


def params(mib):
    return pltpu.CompilerParams(vmem_limit_bytes=mib * 1024 * 1024)


def iota(shape, axis):
    return lax.broadcasted_iota(jnp.int32, shape, axis)


def ones_where(mask):
    return jnp.where(mask, 1.0, 0.0).astype(F32)


def same_atom(atoms, edges):
    return ones_where(lax.rem(iota((atoms, edges), 1), atoms) == iota((atoms, edges), 0))


def edge_row(table):
    slots, atoms = table.shape
    edges = slots * atoms
    spread = dot(table.astype(F32), same_atom(atoms, edges), precision=HIGH)
    mine = lax.div(iota((slots, edges), 1), atoms) == iota((slots, edges), 0)
    return jnp.sum(jnp.where(mine, spread, 0.0), axis=0, keepdims=True)


def to_column(row):
    n = row.shape[1]
    return jnp.sum(jnp.where(iota((n, n), 0) == iota((n, n), 1), row, 0.0), axis=1, keepdims=True)


def onehot(row, height):
    return ones_where(iota((height, row.shape[1]), 0).astype(F32) == row)


def side(array, axis):
    return jnp.concatenate(array, axis=axis)


def paired(value):
    zero = jnp.zeros_like(value)
    return side([side([value, zero], 1), side([zero, value], 1)], 0)


def entry(dtab, row):
    one = dtab[pl.ds(row, 8, stride=0), :]
    return side([one] * (BLOCK // 8), 0)


def rotate_in(block, feats, dtab, store):
    here = pl.ds(pl.multiple_of(block * BLOCK, BLOCK), BLOCK)
    for level in range(LMAX + 1):
        width = 2 * level + 1
        planes = [feats[level * level + col, here, :] for col in range(width)]
        reach = min(level, MMAX)
        for order in range(-reach, reach + 1):
            first = ROWS[level, order]
            acc = entry(dtab, first) * planes[0]
            for col in range(1, width):
                acc = acc + entry(dtab, first + col) * planes[col]
            store(level, order, acc)


def rotate_out(block, load, dtab, store):
    here = pl.ds(pl.multiple_of(block * BLOCK, BLOCK), BLOCK)
    for level in range(LMAX + 1):
        reach = min(level, MMAX)
        orders = range(-reach, reach + 1)
        planes = {order: load(level, order) for order in orders}
        for col in range(2 * level + 1):
            acc = None
            for order in orders:
                term = entry(dtab, ROWS[level, order] + col) * planes[order]
                acc = term if acc is None else acc + term
            store(level * level + col, here, acc)


def rows_at(level, least, height, block):
    return pl.ds(pl.multiple_of((level - least) * height + block * BLOCK, BLOCK), BLOCK)


def place(order, level, height, block):
    least = abs(order)
    return least, rows_at(level, least, height, block), 1 if order < 0 else 0


def joined(ref, chans):
    count, group = ref.shape[-3], ref.shape[-2]
    if len(ref.shape) == 4:
        return [ref[:, level].reshape(count * group, chans) for level in range(count)]
    return [ref[:, :, level].reshape(2 * count * group, chans) for level in range(count)]


def table_kernel(
    after, wigner_hbm, rotation_hbm, w0_hbm, w1_hbm, w2_hbm,
    dtab, w0, w1, w2, t0, t1, t2,
    wigner, rotation, sems,
):
    copies = [
        pltpu.make_async_copy(source, target, sems.at[at])
        for at, (source, target) in enumerate(
            [
                (rotation_hbm, rotation), (wigner_hbm, wigner),
                (w0_hbm, w0), (w1_hbm, w1), (w2_hbm, w2),
            ]
        )
    ]
    for copy in copies:
        copy.start()
    copies[0].wait()
    pick = onehot(edge_row(rotation[...]), wigner.shape[1]).astype(BF16)
    copies[1].wait()
    wig = wigner[...]
    high = wig.astype(BF16)
    rest = wig - high.astype(F32)
    mid = rest.astype(BF16)
    low = (rest - mid.astype(F32)).astype(BF16)
    dtab[...] = dot(high, pick) + dot(mid, pick) + dot(low, pick)
    for copy, ref, out in zip(copies[2:], (w0, w1, w2), (t0, t1, t2)):
        copy.wait()
        chans = ref.shape[-1]
        for level, part in enumerate(joined(ref, chans)):
            out[level * chans : (level + 1) * chans, :] = jnp.transpose(part)


def fetch(rows_of, pick, feats):
    edges = pick.shape[1]
    group = feats.shape[1]
    both = paired(pick).astype(BF16)
    pairs = (K + 1) // 2
    for first in range(0, pairs, 2):
        blocks = [first, min(first + 1, pairs - 1)]
        got = dot(side([rows_of(at) for at in blocks], 0), both, TN)
        for lane, at in enumerate(blocks):
            for row in range(2):
                if 2 * at + row < K:
                    feats[2 * at + row] = got[
                        row * group : (row + 1) * group, lane * edges : (lane + 1) * edges
                    ]


def start_kernel(own, ghosts, source, grad_hbm, dtab, g0, g1, g2, r0, r1, r2, out_grad, feats, held, sem):
    copy = pltpu.make_async_copy(grad_hbm, out_grad, sem)
    copy.start()
    slots, atoms = source.shape
    edges = slots * atoms
    group = out_grad.shape[2]
    pick = onehot(edge_row(source[...]), atoms + ghosts.shape[1])
    fetch(lambda at: side([own[at], ghosts[at]], 0), pick, feats)
    copy.wait()
    both = paired(same_atom(atoms, edges)).astype(BF16)
    for first in range(0, K, 2):
        ks = [first, min(first + 1, K - 1)]
        got = dot(side([out_grad[k] for k in ks], 0), both, TN)
        for at, k in enumerate(ks):
            held[k] = got[:, at * edges : (at + 1) * edges]

    def step(block, carry):
        for values, outs, kind in ((feats, (r0, r1, r2), BF16), (held, (g0, g1, g2), F32)):

            def store(level, order, acc, outs=outs, kind=kind):
                which, rows, half = place(order, level, group, block)
                outs[which][rows, half * edges : (half + 1) * edges] = acc.astype(kind)

            rotate_in(block, values, dtab, store)
        return carry

    lax.fori_loop(0, group // BLOCK, step, 0)


def over_slots(value, slots, combine):
    edges = value.shape[1]
    out = value
    for slot in range(1, slots):
        out = combine(out, pltpu.roll(value, slot * (edges // slots), axis=1))
    return out


def head_sums(value, heads):
    width = value.shape[0] // heads
    sums = [
        jnp.sum(value[at * width : (at + 1) * width], axis=0, keepdims=True) for at in range(heads)
    ]
    return side(sums + [jnp.zeros_like(sums[0])] * (-heads % 8), 0)


def head_spread(value, heads, width):
    return side(
        [jnp.broadcast_to(value[at : at + 1], (width, value.shape[1])) for at in range(heads)], 0
    )


def edge_kernel(heads, shards, *refs):
    own_parts, ghost_parts, refs = refs[: shards - 1], refs[shards - 1 : 2 * shards - 2], refs[2 * shards - 2 :]
    p0, p1, p2, source, counts, dtab, g0, g1, g2, w0, w1, w2, t0, t1, t2, attn, *refs = refs
    own_out, a_out, b_out, v0, v1, v2, feats, r0, r1, r2, d0, d1, d2, dfeats = refs
    slots, atoms = source.shape
    edges = slots * atoms
    chans = w0.shape[-1]
    group = w0.shape[2]
    half = a_out.shape[1]
    table = atoms + 2 * half
    me = lax.axis_index("ch")
    rots = (r0, r1, r2)
    sources = edge_row(source[...])
    pick = onehot(sources, table)

    for least, (ref, part) in enumerate(zip(rots, (p0, p1, p2))):
        for at in range(LMAX + 1 - least):
            there = pl.ds(pl.multiple_of(at * chans + me * group, BLOCK), group)
            ref[there, :] = part[at * group : (at + 1) * group, :]

    for step, (own, ghosts) in enumerate(zip(own_parts, ghost_parts), 1):
        fetch(lambda at: side([own[at], ghosts[at]], 0), pick, feats)
        base = lax.rem(me + step, shards) * group

        def in_step(block, carry):
            def store(level, order, acc):
                least = abs(order)
                lane = edges if order < 0 else 0
                row = (level - least) * chans + base + block * BLOCK
                rots[least][pl.ds(pl.multiple_of(row, BLOCK), BLOCK), lane : lane + edges] = acc.astype(BF16)

            rotate_in(block, feats, dtab, store)
            return carry

        lax.fori_loop(0, group // BLOCK, in_step, 0)

    def weights_of(ref):
        return side(joined(ref, chans), 1)

    y0 = dot(weights_of(w0), r0[...])

    def mixed(ref, rot):
        out = dot(weights_of(ref), rot[...])
        tall = out.shape[0] // 2
        plus = out[:tall, :edges] - out[tall:, edges:]
        minus = out[:tall, edges:] + out[tall:, :edges]
        return side([plus, minus], 1)

    mixes = (y0, mixed(w1, r1), mixed(w2, r2))
    grads = (g0[...], g1[...], g2[...])

    scalar = y0[:group]
    sig = 1.0 / (1.0 + jnp.exp(-scalar))
    vector = to_column(attn[...])
    width = group // heads
    spread = dot(counts[...].astype(F32), same_atom(atoms, edges), precision=HIGH)
    score = head_sums(scalar * sig * vector, heads)
    live = lax.div(iota(score.shape, 1), atoms).astype(F32) < spread
    score = jnp.where(live, score, -1e30)
    top = over_slots(score, slots, jnp.maximum)
    weight = jnp.where(live, jnp.exp(score - top), 0.0)
    weight = weight / over_slots(weight, slots, jnp.add)
    factor = head_spread(weight, heads, width) * sig

    overlap = None
    for grad, mix in zip(grads, mixes):
        product = grad * mix
        for at in range(0, product.shape[0], group):
            for lane in range(0, product.shape[1], edges):
                piece = product[at : at + group, lane : lane + edges]
                overlap = piece if overlap is None else overlap + piece
    dweight = head_sums(overlap * sig, heads)
    mean = over_slots(weight * dweight, slots, jnp.add)
    dscore = head_spread(weight * (dweight - mean), heads, width)
    dscalar = overlap * factor * (1.0 - sig) + dscore * vector * sig * (1.0 + scalar * (1.0 - sig))

    dmix = []
    for grad, mix, out in zip(grads, mixes, (v0, v1, v2)):
        wide = side([factor] * (mix.shape[1] // edges), 1)
        wide = side([wide] * (mix.shape[0] // group), 0)
        out[...] = mix * wide
        dmix.append(grad * wide)
    back0 = side([dmix[0][:group] + dscalar, dmix[0][group:]], 0).astype(BF16)
    d0[...] = dot(t0[...], back0).astype(BF16).astype(F32)
    for ref, value, out in ((t1, dmix[1], d1), (t2, dmix[2], d2)):
        flipped = side([value[:, edges:], -value[:, :edges]], 1)
        stacked = side([value, flipped], 0).astype(BF16)
        out[...] = dot(ref[...], stacked).astype(BF16).astype(F32)

    drots = (d0, d1, d2)

    def out_step(block, carry):
        def load(level, order):
            which, rows, side_no = place(order, level, chans, block)
            return drots[which][rows, side_no * edges : (side_no + 1) * edges]

        def store(k, here, value):
            dfeats[k, here, :] = value.astype(BF16)

        rotate_out(block, load, dtab, store)
        return carry

    lax.fori_loop(0, chans // BLOCK, out_step, 0)

    numbers = sources.astype(jnp.int32)
    turned = atoms + lax.rem(numbers - atoms + parity() * half, 2 * half)
    pick = onehot(jnp.where(numbers < atoms, numbers, turned).astype(F32), table).astype(BF16)
    for first in range(0, K, 2):
        ks = [k for k in (first, first + 1) if k < K]
        got = dot(pick, side([dfeats[k] for k in ks], 0), NT)
        for at, k in enumerate(ks):
            mine = got[:, at * chans : (at + 1) * chans]
            own_out[k] = mine[:atoms]
            a_out[k] = mine[atoms : atoms + half].astype(BF16)
            b_out[k] = mine[atoms + half :].astype(BF16)


def update_kernel(v0, v1, v2, dtab, mine, out, back):
    atoms, group = mine.shape[1], mine.shape[2]
    edges = dtab.shape[1]
    values = (v0, v1, v2)

    def step(block, carry):
        def load(level, order):
            which, rows, side_no = place(order, level, group, block)
            return values[which][rows, side_no * edges : (side_no + 1) * edges]

        def store(k, here, value):
            back[k, here, :] = value.astype(BF16)

        rotate_out(block, load, dtab, store)
        return carry

    lax.fori_loop(0, group // BLOCK, step, 0)
    owner = same_atom(atoms, edges).astype(BF16)
    for k in range(K):
        agg = dot(owner, back[k], NT)
        out[k] = (mine[k].astype(F32) + agg).astype(BF16)


def parity():
    return lax.rem(lax.axis_index("dom"), 2)


def pack_kernel(mine_hbm, ghost_hbm, out, mine, ghost, sems):
    copies = [
        pltpu.make_async_copy(mine_hbm, mine, sems.at[0]),
        pltpu.make_async_copy(ghost_hbm, ghost, sems.at[1]),
    ]
    for copy in copies:
        copy.start()
    for copy in copies:
        copy.wait()
    for at in range(out.shape[0] - 1):
        out[at] = side([mine[2 * at], mine[min(2 * at + 1, K - 1)]], 1)
    slots = ghost[...].astype(F32)
    rest = jnp.zeros((1, out.shape[2] - slots.shape[1]), F32)
    out[out.shape[0] - 1] = jnp.broadcast_to(side([slots, rest], 1), out.shape[1:]).astype(BF16)


def ghost_kernel(after, first, second, ghost, out):
    atoms = first.shape[1]
    slots = ghost.shape[1]
    odd = parity()
    lane = iota((1, slots), 1)
    target = ghost[...] + jnp.where(lane < slots // 2, odd * atoms, (1 - odd) * atoms)
    rows = to_column(target.astype(F32))
    pick = ones_where(iota((slots, 2 * atoms), 1).astype(F32) == rows).astype(BF16)
    for at in range(out.shape[0]):
        out[at] = dot(pick, side([first[at], second[at]], 0)).astype(BF16)


def settle_kernel(shards, own, got_a, got_b, face_a, face_b, out_grad, mine_out, *others):
    group = out_grad.shape[2]
    atoms, chans = own.shape[1:]
    half = got_a.shape[1]
    me = lax.axis_index("ch")
    even = parity() == 0
    slots_a = face_a[face_a.shape[0] - 1][:, : 2 * half].astype(F32)
    slots_b = face_b[face_b.shape[0] - 1][:, : 2 * half].astype(F32)
    asked = side(
        [
            jnp.where(even, slots_a[:, half:], slots_a[:, :half]),
            jnp.where(even, slots_b[:, :half], slots_b[:, half:]),
        ],
        1,
    )
    pick = ones_where(asked == iota((atoms, 2 * half), 0).astype(F32)).astype(BF16)

    def part(value, step):
        wanted = lax.rem(me + step, shards)
        out = value[:, :group]
        for chunk in range(1, shards):
            out = jnp.where(wanted == chunk, value[:, chunk * group : (chunk + 1) * group], out)
        return out

    for first in range(0, K, 2):
        ks = [first, min(first + 1, K - 1)]
        ghosts = side([side([got_a[k], got_b[k]], 0) for k in ks], 1)
        got = dot(pick, ghosts)
        totals = [own[k] + got[:, at * chans : (at + 1) * chans] for at, k in enumerate(ks)]
        for k, total in zip(ks, totals):
            mine_out[k] = part(total, 0) + out_grad[k].astype(F32)
        for step in range(1, shards):
            others[step - 1][first // 2] = side(
                [part(total, step) for total in totals], 1
            ).astype(BF16)


def final_kernel(mine, *refs):
    others, out = refs[:-1], refs[-1]
    group = mine.shape[2]
    for k in range(K):
        lane = (k % 2) * group
        total = mine[k]
        for other in others:
            total = total + other[k // 2].astype(F32)[:, lane : lane + group]
        out[k] = total


def shift(array, axis, by):
    count = lax.axis_size(axis)
    return lax.ppermute(array, axis, [(i, (i + by) % count) for i in range(count)])


def swap(array, first):
    count = lax.axis_size("dom")
    step = [-1, 1] if first else [1, -1]
    return lax.ppermute(array, "dom", [(i, (i + step[i % 2]) % count) for i in range(count)])


def cost(flops, size):
    return pl.CostEstimate(flops=flops, bytes_accessed=size, transcendentals=0)


def on_device(
    node_irreps, out_grad, edge_source, edge_rotation, edge_count, ghost_slot, wigner,
    so2_m0, so2_m1, so2_m2, attn_vector,
):
    group, atoms = node_irreps.shape[1], node_irreps.shape[2]
    shards = lax.axis_size("ch")
    chans = group * shards
    slots = edge_source.shape[0]
    edges = slots * atoms
    heads_here = HEADS // shards
    shape = jax.ShapeDtypeStruct
    mine = jnp.transpose(node_irreps, (0, 2, 1))
    grad = jnp.transpose(out_grad, (0, 2, 1))
    w0 = jnp.transpose(so2_m0, (0, 2, 1, 3))
    w1 = jnp.transpose(so2_m1, (0, 1, 3, 2, 4))
    w2 = jnp.transpose(so2_m2, (0, 1, 3, 2, 4))

    pairs = (K + 1) // 2
    ghosts = ghost_slot.reshape(1, -1)
    half = ghosts.shape[1] // 2
    packed = pl.pallas_call(
        pack_kernel,
        out_shape=shape((pairs + 1, atoms, 2 * group), BF16),
        in_specs=[hbm(), hbm()],
        out_specs=vmem(1)[0],
        scratch_shapes=[
            pltpu.VMEM(mine.shape, BF16),
            pltpu.VMEM(ghosts.shape, jnp.int32),
            pltpu.SemaphoreType.DMA((2,)),
        ],
        compiler_params=params(4),
        name="pack",
    )(pinned(mine), pinned(ghosts))
    face_a = swap(packed, True)
    others = [shift(packed, "ch", -step) for step in range(1, shards)]
    face_b = swap(packed, False)

    shapes = [
        ((LMAX + 1 - least) * group, edges * (1 if least == 0 else 2)) for least in range(MMAX + 1)
    ]
    wide = [
        ((LMAX + 1 - least) * chans, edges * (1 if least == 0 else 2)) for least in range(MMAX + 1)
    ]
    weights = (w0, w1, w2)
    turned = [(wide[i][0], shapes[i][0] * (2 if i else 1)) for i in range(3)]
    dtab, *tables = pl.pallas_call(
        table_kernel,
        out_shape=[shape((wigner.shape[0], edges), F32)]
        + [shape(w.shape, BF16) for w in weights]
        + [shape(t, BF16) for t in turned],
        in_specs=[hbm()] * 6,
        out_specs=vmem(7),
        scratch_shapes=[
            pltpu.VMEM(wigner.shape, F32),
            pltpu.VMEM(edge_rotation.shape, jnp.int32),
            pltpu.SemaphoreType.DMA((5,)),
        ],
        compiler_params=params(16),
        cost_estimate=cost(20_000_000, 4_000_000),
        name="tables",
    )(packed, pinned(wigner), pinned(edge_rotation), *[pinned(w) for w in weights])
    weights, turned = tables[:3], tables[3:]

    ghost_mine = pl.pallas_call(
        ghost_kernel,
        out_shape=shape((pairs, 2 * half, 2 * group), BF16),
        in_specs=[hbm(), *vmem(3)],
        out_specs=vmem(1)[0],
        compiler_params=params(4),
        name="ghosts",
    )(dtab, face_a, face_b, ghosts)
    ghost_others = [shift(ghost_mine, "ch", -step) for step in range(1, shards)]

    own_rows = [(shapes[i][0], shapes[i][1]) for i in range(3)]
    started = pl.pallas_call(
        start_kernel,
        out_shape=[shape(s, F32) for s in shapes]
        + [shape(s, BF16) for s in own_rows]
        + [shape(grad.shape, BF16)],
        in_specs=[*vmem(3), hbm(), *vmem(1)],
        out_specs=vmem(7),
        scratch_shapes=[
            pltpu.VMEM((K, group, edges), F32),
            pltpu.VMEM((K, group, edges), F32),
            pltpu.SemaphoreType.DMA(()),
        ],
        compiler_params=params(16),
        cost_estimate=cost(20_000_000, 4_000_000),
        name="start",
    )(packed, ghost_mine, edge_source, pinned(grad), dtab)
    grads, rotated, grad = started[:3], started[3:6], started[6]

    own, to_a, to_b, *values = pl.pallas_call(
        functools.partial(edge_kernel, heads_here, shards),
        out_shape=[
            shape((K, atoms, chans), F32),
            shape((K, half, chans), BF16),
            shape((K, half, chans), BF16),
        ] + [shape(s, F32) for s in shapes],
        in_specs=vmem(14 + 2 * shards),
        out_specs=vmem(6),
        scratch_shapes=[pltpu.VMEM((K, group, edges), F32)]
        + [pltpu.VMEM(s, BF16) for s in wide]
        + [pltpu.VMEM(s, F32) for s in wide]
        + [pltpu.VMEM((K, chans, edges), BF16)],
        compiler_params=params(24),
        cost_estimate=cost(2_000_000_000, 20_000_000),
        name="edges",
    )(
        *others, *ghost_others, *rotated, edge_source, edge_count.reshape(1, -1),
        dtab, *grads, *weights, *turned, attn_vector.reshape(1, -1),
    )
    got_a = swap(to_a, True)
    got_b = swap(to_b, False)

    updated = pl.pallas_call(
        update_kernel,
        out_shape=shape((K, atoms, group), BF16),
        in_specs=vmem(5),
        out_specs=vmem(1)[0],
        scratch_shapes=[pltpu.VMEM((K, group, edges), BF16)],
        compiler_params=params(8),
        cost_estimate=cost(20_000_000, 4_000_000),
        name="update",
    )(*values, dtab, mine)

    mine_grad, *sent = pl.pallas_call(
        functools.partial(settle_kernel, shards),
        out_shape=[shape((K, atoms, group), F32)]
        + [shape((pairs, atoms, 2 * group), BF16)] * (shards - 1),
        in_specs=vmem(6),
        out_specs=vmem(shards),
        compiler_params=params(8),
        name="settle",
    )(own, got_a, got_b, face_a, face_b, grad)
    mine_grad = pl.pallas_call(
        final_kernel,
        out_shape=shape((K, atoms, group), F32),
        in_specs=vmem(shards),
        out_specs=vmem(1)[0],
        compiler_params=params(4),
        name="final",
    )(mine_grad, *[shift(sent[step - 1], "ch", step) for step in range(1, shards)])
    return (jnp.transpose(updated, (0, 2, 1)), jnp.transpose(mine_grad, (0, 2, 1)))


def solution(mesh):
    placed = (
        P(None, "ch", "dom"), P(None, "ch", "dom"), P(None, "dom"), P(None, "dom"), P("dom"),
        P("dom"), P(None, "dom"), P(None, "ch", None, None), P(None, None, "ch", None, None),
        P(None, None, "ch", None, None), P("ch"),
    )
    return jax.shard_map(
        on_device,
        mesh=mesh,
        in_specs=placed,
        out_specs=(P(None, "ch", "dom"), P(None, "ch", "dom")),
        check_vma=False,
    )
```
